16 devices in a mesh: data: 16 (over z, y, x, core).
Axes of the slice: x: 2, y: 2, z: 2, core: 2. Of those that a mesh axis runs over, the one named last changes fastest.
Arguments:
- x_in: bfloat16 [32768, 1024], P('data')
- dy_in: bfloat16 [32768, 1024], P('data')
- weights: bfloat16 [4, 1024, 1024], replicated
- a_old: float32 [4096, 1024], P('data')
- s_old: float32 [4096, 1024], P('data')
- a_inv: float32 [4096, 1024], P('data')
- s_inv: float32 [4, 1024, 1024], replicated
Outputs:
- output 1: float32 [4, 1024, 1024], replicated
- output 2: float32 [4096, 1024], P('data')
- output 3: float32 [4096, 1024], P('data')
All inputs are finite; a program needn't handle non-finite values.
Results may differ from the reference program's by a relative error of at most 0.00181429.
Values are sent between devices in bfloat16 or wider.
A program may use at most 1 GiB of HBM per device.

```python
import functools
import jax
import jax.numpy as jnp

D = 1024
LAYERS = 4
TOKENS = 2048
SHARDS = 16
LOW_RANK = 64
BATCH_TOTAL = TOKENS * SHARDS
FACTOR_DECAY = 0.75


def spd_stack(rng_key, base_diag, gram_scale):
    low_rank = jax.random.normal(rng_key, (LAYERS, D, LOW_RANK), jnp.float32)
    gram_mat = jnp.einsum("lir,ljr->lij", low_rank, low_rank)
    gram_mat = 0.5 * (gram_mat + jnp.swapaxes(gram_mat, 1, 2))
    return gram_scale * gram_mat + base_diag * jnp.eye(D, dtype=jnp.float32)


def shard_rows(rng_key, spread):
    key_raw, key_mean, key_scale = jax.random.split(rng_key, 3)
    raw_rows = jax.random.normal(key_raw, (SHARDS, TOKENS, D), jnp.float32)
    offset = 0.7 * jax.random.normal(key_mean, (SHARDS, 1, D), jnp.float32)
    row_scale = jnp.exp(spread * jax.random.normal(key_scale, (SHARDS, 1, 1), jnp.float32))
    return ((raw_rows + offset) * row_scale).reshape(BATCH_TOTAL, D).astype(jnp.bfloat16)


def setup_inputs(seed: int = 0) -> dict:
    key_list = jax.random.split(jax.random.key(seed), 7)
    weights = jax.random.normal(key_list[2], (LAYERS, D, D), jnp.float32) * D ** -0.5
    inv_scale = (LOW_RANK * D) ** -0.5
    return {
        "x_in": shard_rows(key_list[0], 0.5),
        "dy_in": shard_rows(key_list[1], 0.5),
        "weights": weights.astype(jnp.bfloat16),
        "a_old": spd_stack(key_list[3], 0.5, 1.0 / LOW_RANK).reshape(LAYERS * D, D),
        "s_old": spd_stack(key_list[4], 0.5, 1.0 / LOW_RANK).reshape(LAYERS * D, D),
        "a_inv": spd_stack(key_list[5], 0.5, inv_scale).reshape(LAYERS * D, D),
        "s_inv": spd_stack(key_list[6], 0.5, inv_scale),
    }


def gelu_grad(pre_act, d_act):
    pullback = jax.vjp(functools.partial(jax.nn.gelu, approximate=True), pre_act.astype(jnp.float32))[1]
    return pullback(d_act.astype(jnp.float32))[0].astype(jnp.bfloat16)


def reference(x_in, dy_in, weights, a_old, s_old, a_inv, s_inv):
    layer_inputs = [x_in]
    pre_acts = []
    for layer_id in range(LAYERS - 1):
        pre_act = jnp.dot(layer_inputs[layer_id], weights[layer_id], preferred_element_type=jnp.float32).astype(jnp.bfloat16)
        pre_acts.append(pre_act)
        layer_inputs.append(jax.nn.gelu(pre_act.astype(jnp.float32), approximate=True).astype(jnp.bfloat16))
    out_grads = [dy_in] * LAYERS
    for layer_id in range(LAYERS - 1, 0, -1):
        d_act = jnp.dot(out_grads[layer_id], weights[layer_id].T, preferred_element_type=jnp.float32).astype(jnp.bfloat16)
        out_grads[layer_id - 1] = gelu_grad(pre_acts[layer_id - 1], d_act)
    a_facs = []
    s_facs = []
    updates = []
    for layer_id in range(LAYERS):
        h_in = layer_inputs[layer_id]
        g_out = out_grads[layer_id]
        a_facs.append(jnp.dot(h_in.T, h_in, preferred_element_type=jnp.float32) / BATCH_TOTAL)
        s_facs.append(jnp.dot(g_out.T, g_out, preferred_element_type=jnp.float32) / BATCH_TOTAL)
        w_grad = jnp.dot(h_in.T, g_out, preferred_element_type=jnp.float32) / BATCH_TOTAL
        a_inv_layer = a_inv[layer_id * D:(layer_id + 1) * D]
        updates.append(jnp.dot(a_inv_layer, jnp.dot(w_grad, s_inv[layer_id])))
    a_new = FACTOR_DECAY * a_old + (1.0 - FACTOR_DECAY) * jnp.concatenate(a_facs, axis=0)
    s_new = FACTOR_DECAY * s_old + (1.0 - FACTOR_DECAY) * jnp.concatenate(s_facs, axis=0)
    return (jnp.stack(updates), a_new, s_new)
```

```python
import functools
import jax
import jax.numpy as jnp
from jax import lax
from jax.experimental import pallas as pl
from jax.experimental.pallas import tpu as pltpu
from jax.sharding import PartitionSpec as P

FACTOR_DECAY = 0.75
PRECISE = lax.Precision.HIGHEST
MESH = pl.DeviceIdType.MESH
PAD = 16
CORE, X, Y, Z = 1, 2, 4, 8
PARTS = ((0, 384, (X, Y, Z)), (384, 384, (Y, Z, X)), (768, 256, (Z, X, Y)))


def gelu_grad(pre_act, d_act):
    pullback = jax.vjp(functools.partial(jax.nn.gelu, approximate=True), pre_act.astype(jnp.float32))[1]
    return pullback(d_act.astype(jnp.float32))[0].astype(jnp.bfloat16)


def cross_rows(left_op, right_op):
    return jnp.einsum("bi,bj->ij", left_op, right_op, preferred_element_type=jnp.float32)


def encode(value, top):
    w = value * (131072.0 / top)
    w2 = w * w
    return (w * w2 * (w2 * w2)).astype(jnp.bfloat16)


def decode(code, top):
    y = code.astype(jnp.float32)
    mag = jnp.abs(y)
    root = jnp.exp(jnp.log(jnp.where(mag > 0.0, mag, 1.0)) * (1.0 / 7.0)) * (top * (1.0 / 131072.0))
    return jnp.where(y > 0.0, root, jnp.where(y < 0.0, -root, 0.0))


def block_top(value):
    top = jnp.maximum(jnp.max(jnp.abs(value)), 1e-30) * 1.01
    return top.astype(jnp.bfloat16).astype(jnp.float32)


def tail_kernel(g_ref, ainv_ref, sinv_hbm, u_ref, sinv, t_all, t_out, t_in, own_sem, t_send, t_recv, u_send, u_recv):
    rows = g_ref.shape[0]
    width = g_ref.shape[1]
    me = lax.axis_index("data")
    core = lax.rem(me, 2)
    xx = lax.rem(me // 2, 2)
    yy = lax.rem(me // 4, 2)
    zz = me // 8
    off = {CORE: 1 - 2 * core, X: 2 * (1 - 2 * xx), Y: 4 * (1 - 2 * yy), Z: 8 * (1 - 2 * zz)}

    load = pltpu.make_async_copy(sinv_hbm.at[me // 4], sinv, own_sem)
    load.start()
    barrier = pltpu.get_barrier_semaphore()
    for d in (CORE, X, Y, Z):
        pl.semaphore_signal(barrier, inc=1, device_id=(me + off[d],), device_id_type=MESH)
    pl.semaphore_wait(barrier, 4)
    load.wait()

    own = 2 * xx + core
    chunk = 256

    @pl.loop(0, width // chunk)
    def _(j):
        cols = pl.ds(pl.multiple_of(j * chunk, chunk), chunk)
        t_all[own, :, cols] = jnp.dot(g_ref[...], sinv[:, cols], precision=PRECISE)

    t_top = block_top(t_all[own])
    t_out[pl.ds(0, rows), :] = encode(t_all[own], t_top)
    t_out[pl.ds(rows, PAD), :] = jnp.full((PAD, width), t_top, jnp.bfloat16)

    def send(src, dst, d, sems, i):
        copy = pltpu.make_async_remote_copy(
            src_ref=src, dst_ref=dst, send_sem=sems[0].at[i], recv_sem=sems[1].at[i],
            device_id=(me + off[d],), device_id_type=MESH)
        copy.start()
        return copy

    t_sems = (t_send, t_recv)
    across = send(t_out, t_in.at[0], X, t_sems, 0)
    beside = send(t_out, t_in.at[1], CORE, t_sems, 1)
    across.wait_recv()
    diag = send(t_in.at[0], t_in.at[2], CORE, t_sems, 2)
    beside.wait_recv()
    diag.wait_recv()

    def take(code_ref):
        return decode(code_ref[pl.ds(0, rows), :], code_ref[pl.ds(rows, 1), pl.ds(0, 1)].astype(jnp.float32))

    t_all[2 * (1 - xx) + core] = take(t_in.at[0])
    t_all[2 * xx + 1 - core] = take(t_in.at[1])
    t_all[2 * (1 - xx) + 1 - core] = take(t_in.at[2])

    u_rows = sinv

    @pl.loop(0, width // chunk)
    def _(j):
        cols = pl.ds(pl.multiple_of(j * chunk, chunk), chunk)
        acc = jnp.zeros((rows, chunk), jnp.float32)
        for k in range(4):
            acc += jnp.dot(ainv_ref[:, k * rows:(k + 1) * rows], t_all[k, :, cols], precision=PRECISE)
        u_rows[pl.ds(0, rows), cols] = acc

    u_top = block_top(u_rows[pl.ds(0, rows), :])
    u_ref[me, pl.ds(0, rows), :] = encode(u_rows[pl.ds(0, rows), :], u_top)
    u_ref[me, pl.ds(rows, PAD), :] = jnp.full((PAD, width), u_top, jnp.bfloat16)
    across.wait_send()
    beside.wait_send()
    diag.wait_send()

    u_sems = (u_send, u_recv)
    sent = []

    def pass_on(slot, part, d, i):
        first, size, _ = PARTS[part]
        ref = u_ref.at[slot, :, pl.ds(first, size)]
        copy = send(ref, ref, d, u_sems, part * 15 + i)
        sent.append(copy)
        return copy

    slots = [[me] for _ in PARTS]
    waits = [[] for _ in PARTS]
    core_i = [7 for _ in PARTS]
    last = []
    for stage in range(3):
        for part, (_, _, order) in enumerate(PARTS):
            for copy in waits[part]:
                copy.wait_recv()
            d = order[stage]
            base = (1 << stage) - 1
            waits[part] = [pass_on(s, part, d, base + k) for k, s in enumerate(slots[part])]
            fresh = slots[part] if stage == 0 else slots[part][len(slots[part]) // 2:]
            for s in fresh:
                last.append(pass_on(s, part, CORE, core_i[part]))
                core_i[part] += 1
            slots[part] = slots[part] + [s + off[d] for s in slots[part]]
    for part in range(len(PARTS)):
        for copy in waits[part]:
            copy.wait_recv()
        for s in slots[part][4:]:
            last.append(pass_on(s, part, CORE, core_i[part]))
            core_i[part] += 1
    for copy in last:
        copy.wait_recv()
    for copy in sent:
        copy.wait_send()


def tail(g_rows, a_inv_rows, s_inv, n_dev):
    rows, width = g_rows.shape
    block = (rows + PAD, width)
    vmem = pl.BlockSpec(memory_space=pltpu.VMEM)
    return pl.pallas_call(
        tail_kernel,
        out_shape=jax.ShapeDtypeStruct((n_dev,) + block, jnp.bfloat16),
        in_specs=[vmem, vmem, pl.BlockSpec(memory_space=pl.ANY)],
        out_specs=vmem,
        scratch_shapes=[
            pltpu.VMEM((width, width), jnp.float32),
            pltpu.VMEM((4, rows, width), jnp.float32),
            pltpu.VMEM(block, jnp.bfloat16),
            pltpu.VMEM((3,) + block, jnp.bfloat16),
            pltpu.SemaphoreType.DMA,
            pltpu.SemaphoreType.DMA((3,)),
            pltpu.SemaphoreType.DMA((3,)),
            pltpu.SemaphoreType.DMA((45,)),
            pltpu.SemaphoreType.DMA((45,)),
        ],
        compiler_params=pltpu.CompilerParams(collective_id=0, has_side_effects=True, vmem_limit_bytes=48 * 2**20),
        cost_estimate=pl.CostEstimate(flops=6 * 4 * rows * width * width, bytes_accessed=20 * 2**20, transcendentals=0),
    )(g_rows, a_inv_rows, s_inv)


def solution(mesh):
    n_dev = mesh.shape["data"]

    def device_step(x_loc, dy_loc, weights, a_old_rows, s_old_rows, a_inv_rows, s_inv):
        n_layers, width = weights.shape[0], weights.shape[1]
        rows = a_old_rows.shape[0]
        batch_total = x_loc.shape[0] * n_dev
        me = lax.axis_index("data")
        bit = {CORE: me % 2, X: (me // 2) % 2, Y: (me // 4) % 2, Z: me // 8}

        def swap(value, d, wire):
            out = lax.ppermute(value.astype(wire), "data", [(p, p ^ d) for p in range(n_dev)])
            return out.astype(jnp.float32)

        def gather_pair(full, wires):
            blocks = full.reshape(2, 2, rows, width)
            theirs = lax.dynamic_index_in_dim(blocks, 1 - bit[CORE], 1, keepdims=False)
            mine = lax.dynamic_index_in_dim(blocks, bit[CORE], 1, keepdims=False)
            got = swap(theirs, CORE, jnp.float32)

            def pick(i):
                return lax.dynamic_index_in_dim(mine, i, 0, keepdims=False) + lax.dynamic_index_in_dim(got, i, 0, keepdims=False)

            return pick(bit[X]) + swap(pick(1 - bit[X]), X, wires[0])

        def gather_plane(layers, wires):
            half = width // 2
            pieces = []
            for first, (d1, d2) in ((0, (Z, Y)), (half, (Y, Z))):
                part = [v[:, first:first + half] for v in layers]
                if d1 == Z:
                    pairs = [(part[0], part[2]), (part[1], part[3])]
                else:
                    pairs = [(part[0], part[1]), (part[2], part[3])]
                low = bit[d1] == 0
                send = jnp.stack([jnp.where(low, hi, lo) for lo, hi in pairs])
                keep = jnp.stack([jnp.where(low, lo, hi) for lo, hi in pairs])
                both = keep + swap(send, d1, wires[1])
                low = bit[d2] == 0
                out = jnp.where(low, both[0], both[1]) + swap(jnp.where(low, both[1], both[0]), d2, wires[2])
                pieces.append(out)
            return jnp.concatenate(pieces, axis=1)

        a_wires = (jnp.bfloat16, jnp.bfloat16, jnp.float32)
        g_wires = (jnp.bfloat16, jnp.float32, jnp.float32)

        layer_inputs, pre_acts, a_parts = [x_loc], [], []
        for layer_id in range(n_layers - 1):
            pre_act = jnp.dot(layer_inputs[layer_id], weights[layer_id], preferred_element_type=jnp.float32).astype(jnp.bfloat16)
            pre_acts.append(pre_act)
            layer_inputs.append(jax.nn.gelu(pre_act.astype(jnp.float32), approximate=True).astype(jnp.bfloat16))
        out_grads = [dy_loc] * n_layers
        for layer_id in range(n_layers - 1, 0, -1):
            d_act = jnp.einsum("bj,ij->bi", out_grads[layer_id], weights[layer_id], preferred_element_type=jnp.float32).astype(jnp.bfloat16)
            out_grads[layer_id - 1] = gelu_grad(pre_acts[layer_id - 1], d_act)

        a_parts = [gather_pair(cross_rows(h_in, h_in), a_wires) for h_in in layer_inputs]
        w_parts = [gather_pair(cross_rows(h_in, g_out), g_wires) for h_in, g_out in zip(layer_inputs, out_grads)]
        w_own = gather_plane(w_parts, g_wires)
        s_parts = [gather_pair(cross_rows(g_out, g_out), a_wires) for g_out in out_grads]
        a_own = gather_plane(a_parts, a_wires)
        s_own = gather_plane(s_parts, a_wires)

        u_code = tail(w_own * (1.0 / batch_total), a_inv_rows, s_inv, n_dev)
        u_full = decode(u_code[:, :rows], u_code[:, rows:rows + 1, :1].astype(jnp.float32)).reshape(n_layers, width, width)
        grow = (1.0 - FACTOR_DECAY) / batch_total
        a_new = FACTOR_DECAY * a_old_rows + grow * a_own
        s_new = FACTOR_DECAY * s_old_rows + grow * s_own
        return u_full, a_new, s_new

    row_spec = P("data", None)
    return jax.shard_map(
        device_step,
        mesh=mesh,
        in_specs=(row_spec, row_spec, P(), row_spec, row_spec, row_spec, P()),
        out_specs=(P(), row_spec, row_spec),
        check_vma=False,
    )
```
